16 devices in a mesh: rep: 4 (over y, z, core), dp: 4 (over x).
Axes of the slice: x: 4, y: 2, z: 1, core: 2. Of those that a mesh axis runs over, the one named last changes fastest.
The devices are a block of a 4x4x8 slice.
Arguments:
- x: bfloat16 [16, 2048, 768], P(('rep', 'dp')), parts along dimension 0
- dy: bfloat16 [16, 2048, 768], P(('rep', 'dp')), parts along dimension 0
- w_gate: bfloat16 [2, 768, 3072], replicated
- w_up: bfloat16 [2, 768, 3072], replicated
- w_down: bfloat16 [2, 3072, 768], replicated
- m_w_gate: float32 [2, 768, 3072], replicated
- m_w_up: float32 [2, 768, 3072], replicated
- m_w_down: float32 [2, 3072, 768], replicated
- v_w_gate: float32 [2, 768, 3072], replicated
- v_w_up: float32 [2, 768, 3072], replicated
- v_w_down: float32 [2, 3072, 768], replicated
Outputs:
- output 1: bfloat16 [8, 768, 3072], P('rep'), parts along dimension 0
- output 2: bfloat16 [8, 768, 3072], P('rep'), parts along dimension 0
- output 3: bfloat16 [8, 3072, 768], P('rep'), parts along dimension 0
- output 4: float32 [8, 768, 3072], P('rep'), parts along dimension 0
- output 5: float32 [8, 768, 3072], P('rep'), parts along dimension 0
- output 6: float32 [8, 3072, 768], P('rep'), parts along dimension 0
- output 7: float32 [8, 768, 3072], P('rep'), parts along dimension 0
- output 8: float32 [8, 768, 3072], P('rep'), parts along dimension 0
- output 9: float32 [8, 3072, 768], P('rep'), parts along dimension 0
There are 4 independent parts. The reference program is written for one: setup_inputs(seed, part) draws one part's arguments, and reference() takes and returns one part's arrays. A program takes and returns all parts, laid end to end along the dimension named above; an argument that names none is the same for every part.
All inputs are finite; a program needn't handle non-finite values.
Results may differ from the reference program's by a relative error of at most 0.022.
Values are sent between devices in bfloat16 or wider.
A program may use at most 768 MiB of HBM per device.

```python
import jax
import jax.numpy as jnp
from jax import lax

SEQUENCES = 4
TOKENS = 2048
D = 768
FF = 3072
LAYERS = 2
NAMES = ("w_gate", "w_up", "w_down")
SHAPES = {"w_gate": (LAYERS, D, FF), "w_up": (LAYERS, D, FF), "w_down": (LAYERS, FF, D)}


def bump(key, n, height):
    away = (jnp.arange(n, dtype=jnp.int32) - jax.random.randint(key, (), 0, n, jnp.int32)) % n
    return jnp.where(away < n // 8, height, 1.0)


def together(key, own, strength):
    shared = jax.random.normal(key, own.shape[1:], jnp.float32)
    return (own + strength * shared) * lax.rsqrt(1 + strength * strength)


def setup_inputs(seed: int = 0, part: int = 0) -> dict:
    kx, kdy, ka, kb, kz, kf, kh, kl, *keys = jax.random.split(jax.random.key(seed), 8 + 3 * len(NAMES))
    kx, kdy, ka, kb = (jax.random.fold_in(k, part) for k in (kx, kdy, ka, kb))
    kw, km, kv = (keys[i::3] for i in range(3))
    shape = (SEQUENCES, TOKENS, D)
    much_x, much_dy = jax.random.uniform(kz, (2,), jnp.float32, 0.0, 1.0)
    loud = 2.0 ** jax.random.uniform(jax.random.fold_in(kz, 1), (), jnp.float32, -1.0, 2.0)
    layers = 2.0 ** jax.random.uniform(kl, (LAYERS, 1, 1), jnp.float32, -1.0, 1.0)
    x = together(ka, jax.random.normal(kx, shape, jnp.float32), much_x) * bump(kf, D, 4.0)
    dy = together(kb, jax.random.normal(kdy, shape, jnp.float32), much_dy)
    drawn = {"x": x.astype(jnp.bfloat16), "dy": (loud * dy * (SEQUENCES * TOKENS) ** -0.5).astype(jnp.bfloat16)}
    for key, name in zip(kw, NAMES, strict=True):
        w = jax.random.normal(key, SHAPES[name], jnp.float32) * SHAPES[name][1] ** -0.5
        drawn[name] = (w * {"w_gate": 1.0, "w_up": bump(kh, FF, 4.0), "w_down": layers}[name]).astype(jnp.bfloat16)
    for key, name in zip(km, NAMES, strict=True):
        drawn[f"m_{name}"] = 0.1 * jax.random.normal(key, SHAPES[name], jnp.float32)
    for key, name in zip(kv, NAMES, strict=True):
        drawn[f"v_{name}"] = jax.random.uniform(key, SHAPES[name], jnp.float32, 0.005, 0.015)
    return drawn


def matmul(a, w):
    return jnp.dot(a, w, preferred_element_type=jnp.float32).astype(jnp.bfloat16)


def normed(h):
    wide = h.astype(jnp.float32)
    scale = lax.rsqrt(jnp.mean(wide**2, -1, keepdims=True) + 1e-6)
    return (wide * scale).astype(jnp.bfloat16)


def layer(h, w):
    a = normed(h)
    gate = jnp.dot(a, w["w_gate"], preferred_element_type=jnp.float32)
    up = jnp.dot(a, w["w_up"], preferred_element_type=jnp.float32)
    return h + matmul((jax.nn.silu(gate) * up).astype(jnp.bfloat16), w["w_down"])


def adamw(w, m, v, g):
    m = 0.9 * m + 0.1 * g
    v = 0.95 * v + 0.05 * g * g
    step = m * lax.rsqrt(v + 1e-8) + 0.1 * w
    return (w - 0.02 * step).astype(jnp.bfloat16), m, v


def stack(weights, h):
    return lax.scan(lambda h, w: (layer(h, w), None), h, weights)[0]


def reference(x, dy, w_gate, w_up, w_down, m_w_gate, m_w_up, m_w_down, v_w_gate, v_w_up, v_w_down):
    weights = dict(zip(NAMES, (w_gate, w_up, w_down), strict=True))

    def take(so_far, sequence):
        h, by_y = sequence
        _, back = jax.vjp(lambda w: stack(w, h), weights)
        return jax.tree.map(lambda total, term: total + term.astype(jnp.float32), so_far, back(by_y)[0]), None

    none_yet = {name: jnp.zeros(w.shape, jnp.float32) for name, w in weights.items()}
    by_weights, _ = lax.scan(take, none_yet, (x, dy))
    gradients = [by_weights[name].astype(jnp.bfloat16).astype(jnp.float32) for name in NAMES]
    new = [
        adamw(w.astype(jnp.float32), m, v, g)
        for w, m, v, g in zip((w_gate, w_up, w_down), (m_w_gate, m_w_up, m_w_down), (v_w_gate, v_w_up, v_w_down), gradients, strict=True)
    ]
    return tuple(one[which] for which in range(3) for one in new)
```

```python
import functools

import jax
import jax.numpy as jnp
from jax import lax
from jax.experimental import pallas as pl
from jax.experimental.pallas import tpu as pltpu
from jax.sharding import PartitionSpec as P


BF16, F32 = jnp.bfloat16, jnp.float32
TOKEN_BLOCK = 512
HIDDEN_BLOCK = 512
PIECE = 256
GROUP = 2
VMEM = 67043328


def nn(a, b):
    return lax.dot_general(a, b, (((1,), (0,)), ((), ())), preferred_element_type=F32)


def nt(a, b):
    return lax.dot_general(a, b, (((1,), (1,)), ((), ())), preferred_element_type=F32)


def scale_of(wide):
    return lax.rsqrt(jnp.mean(wide * wide, -1, keepdims=True) + 1e-6)


def call(kernel, after, ins, in_specs, out_specs, out_shape, *, grid, half=None, scratch=(), aliases=None, cost=0):
    after = [] if after is None else [after]
    scalars = [] if half is None else [half]
    first, last = len(scalars) + len(ins), len(scalars) + len(ins) + len(after)

    def body(*refs):
        kernel(*refs[len(scalars) : first], *refs[last:])

    return pl.pallas_call(
        body,
        grid_spec=pltpu.PrefetchScalarGridSpec(
            num_scalar_prefetch=len(scalars),
            grid=grid,
            in_specs=[*in_specs, *[pl.BlockSpec(memory_space=pl.ANY)] * len(after)],
            out_specs=out_specs,
            scratch_shapes=scratch,
        ),
        out_shape=out_shape,
        input_output_aliases=aliases or {},
        compiler_params=pltpu.CompilerParams(vmem_limit_bytes=VMEM, dimension_semantics=("arbitrary",)),
        cost_estimate=pl.CostEstimate(flops=1, bytes_accessed=cost, transcendentals=0),
    )(*scalars, *ins, *after)


def shape(*dims, dtype=BF16):
    return jax.ShapeDtypeStruct(dims, dtype)


def weight_specs(layer, d, hidden):
    once = pl.Buffered(1)
    return [
        pl.BlockSpec((None, d, hidden), lambda i: (layer, 0, 0), pipeline_mode=once),
        pl.BlockSpec((None, d, hidden), lambda i: (layer, 0, 0), pipeline_mode=once),
        pl.BlockSpec((None, hidden, d), lambda i: (layer, 0, 0), pipeline_mode=once),
    ]


def normed(h_ref, a_ref, at_ref):
    wide = h_ref[...].astype(F32)
    a = wide * scale_of(wide)
    a_ref[...] = a.astype(BF16)
    at_ref[...] = a.T.astype(BF16)


def forward_kernel(h_ref, wg_ref, wu_ref, wd_ref, a_ref, at_ref, out_ref):
    normed(h_ref, a_ref, at_ref)
    a = a_ref[...]
    hidden = wg_ref.shape[1]
    bf = min(HIDDEN_BLOCK, hidden)
    acc = None
    for j in range(hidden // bf):
        cols = pl.ds(j * bf, bf)
        g = nn(a, wg_ref[:, cols])
        u = nn(a, wu_ref[:, cols])
        act = (g * jax.nn.sigmoid(g) * u).astype(BF16)
        part = nn(act, wd_ref[cols, :])
        acc = part if acc is None else acc + part
    out_ref[...] = (h_ref[...].astype(F32) + acc.astype(BF16).astype(F32)).astype(BF16)


def forward(h, weights, layer, after):
    t, d = h.shape
    tm = min(TOKEN_BLOCK, t)
    row = pl.BlockSpec((tm, d), lambda i: (i, 0))
    col = pl.BlockSpec((d, tm), lambda i: (0, i))
    return call(
        forward_kernel,
        after,
        (h, *weights),
        [row, *weight_specs(layer, d, weights[0].shape[2])],
        [row, col, row],
        [shape(t, d), shape(d, t), shape(t, d)],
        grid=(t // tm,),
    )


def norm(h, after):
    t, d = h.shape
    tm = min(TOKEN_BLOCK, t)
    row = pl.BlockSpec((tm, d), lambda i: (i, 0))
    col = pl.BlockSpec((d, tm), lambda i: (0, i))
    return call(normed, after, (h,), [row], [row, col], [shape(t, d), shape(d, t)], grid=(t // tm,))


def turn_kernel(x_ref, xt_ref):
    xt_ref[...] = x_ref[...].T


def turn(x, after):
    t, d = x.shape
    tm = min(TOKEN_BLOCK, t)
    row = pl.BlockSpec((tm, d), lambda i: (i, 0))
    col = pl.BlockSpec((d, tm), lambda i: (0, i))
    return call(turn_kernel, after, (x,), [row], col, shape(d, t), grid=(t // tm,))


def gates(g, u, dact):
    s = jax.nn.sigmoid(g)
    silu = g * s
    act = (silu * u).astype(BF16)
    dact = dact.astype(BF16).astype(F32)
    dg = (dact * u * (s + silu * (1.0 - s))).astype(BF16)
    du = (dact * silu).astype(BF16)
    return act, dg, du


def data_kernel(h_ref, a_ref, dy_ref, wg_ref, wu_ref, wd_ref, dh_ref, dht_ref):
    a, dy = a_ref[...], dy_ref[...]
    hidden = wg_ref.shape[1]
    bf = min(HIDDEN_BLOCK, hidden)

    def three(j):
        cols = pl.ds(j * bf, bf)
        return nn(a, wg_ref[:, cols]), nn(a, wu_ref[:, cols]), nt(dy, wd_ref[cols, :])

    acc, now = None, three(0)
    for j in range(hidden // bf):
        cols = pl.ds(j * bf, bf)
        _, dg, du = gates(*now)
        if (j + 1) * bf < hidden:
            now = three(j + 1)
        part = nt(dg, wg_ref[:, cols]) + nt(du, wu_ref[:, cols])
        acc = part if acc is None else acc + part
    da = acc.astype(BF16).astype(F32)
    wide = h_ref[...].astype(F32)
    scale = scale_of(wide)
    inner = jnp.mean(da * wide, -1, keepdims=True)
    back = (scale * da - wide * (scale * scale * scale * inner)).astype(BF16)
    dh = dy.astype(F32) + back.astype(F32)
    dh_ref[...] = dh.astype(BF16)
    dht_ref[...] = dh.T.astype(BF16)


def data_gradient(h, a, dy, weights, layer, after):
    t, d = h.shape
    tm = min(TOKEN_BLOCK, t)
    row = pl.BlockSpec((tm, d), lambda i: (i, 0))
    col = pl.BlockSpec((d, tm), lambda i: (0, i))
    return call(
        data_kernel,
        after,
        (h, a, dy, *weights),
        [row, row, row, *weight_specs(layer, d, weights[0].shape[2])],
        [row, col],
        [shape(t, d), shape(d, t)],
        grid=(t // tm,),
    )


def weight_kernel(*refs):
    own, other, (wg_ref, wu_ref, wd_ref), outs, acc_ref = refs[:4], refs[4:8], refs[8:11], refs[11:-1], refs[-1]
    step = pl.program_id(0)

    @pl.when(step == 0)
    def _():
        acc_ref[...] = jnp.zeros_like(acc_ref)

    wg, wu, wd = wg_ref[...], wu_ref[...], wd_ref[...]
    for a_ref, at_ref, dy_ref, dyt_ref in (own, other):
        a, dy = a_ref[...], dy_ref[...]
        act, dg, du = gates(nn(a, wg), nn(a, wu), nt(dy, wd))
        at, dyt = at_ref[...], dyt_ref[...]
        acc_ref[0] += nn(at, dg)
        acc_ref[1] += nn(at, du)
        acc_ref[2] += nn(dyt, act)

    @pl.when(step == pl.num_programs(0) - 1)
    def _():
        for k, out_ref in enumerate(outs):
            out_ref[...] = acc_ref[:, :, k * PIECE : (k + 1) * PIECE].astype(BF16)


def weight_gradient(half, own, other, weights, layer, start, count, after):
    t, d = own[0].shape
    total = weights[0].shape[2] // (2 * PIECE)
    tm = min(TOKEN_BLOCK, t)
    row = pl.BlockSpec((tm, d), lambda i, half: (i, 0))
    col = pl.BlockSpec((d, tm), lambda i, half: (0, i))
    width = count * PIECE
    at = lambda half: (half[0] * total + start) // count
    across = pl.BlockSpec((None, d, width), lambda i, half: (layer, 0, at(half)))
    down = pl.BlockSpec((None, width, d), lambda i, half: (layer, at(half), 0))
    return call(
        weight_kernel,
        after,
        (*own, *other, *weights),
        [row, col, row, col] * 2 + [across, across, down],
        [pl.BlockSpec((3, d, PIECE), lambda i, half: (0, 0, 0))] * count,
        [shape(3, d, PIECE)] * count,
        grid=(t // tm,),
        half=half,
        scratch=[pltpu.VMEM((3, d, width), F32)],
    )


def merge_kernel(part_ref, came_ref, out_ref):
    out_ref[...] = (part_ref[...].astype(F32) + came_ref[...].astype(F32)).astype(BF16)


def merge(part, came, after):
    spec = pl.BlockSpec((1, *part.shape[1:]), lambda i: (i, 0, 0))
    return call(merge_kernel, after, (part, came), [spec] * 2, spec, shape(*part.shape), grid=(part.shape[0],))


def adamw_kernel(count, *refs):
    gs, ins, outs, token_ref = refs[:count], refs[count : count + 9], refs[-10:-1], refs[-1]
    token_ref[...] = jnp.zeros_like(token_ref)
    for k in range(3):
        g = jnp.concatenate([g_ref[k].astype(F32) for g_ref in gs], 1)
        if k == 2:
            g = g.T
        w = ins[k][...].astype(F32)
        m = 0.9 * ins[3 + k][...] + 0.1 * g
        v = 0.95 * ins[6 + k][...] + 0.05 * g * g
        step = m * lax.rsqrt(v + 1e-8) + 0.1 * w
        outs[k][...] = (w - 0.02 * step).astype(BF16)
        outs[3 + k][...] = m
        outs[6 + k][...] = v


def adamw(half, gs, arrays, so_far, layer, start, after):
    _, d, _ = gs[0].shape
    count = len(gs)
    total = arrays[0].shape[2] // (2 * PIECE)
    rows = min(256, d)
    width = count * PIECE
    at = lambda half: (half[0] * total + start) // count
    across = pl.BlockSpec((None, rows, width), lambda i, half: (layer, i, at(half)))
    down = pl.BlockSpec((None, width, rows), lambda i, half: (layer, at(half), i))
    nine = [across, across, down] * 3
    kept = [] if so_far is None else list(so_far)
    return call(
        functools.partial(adamw_kernel, count),
        after,
        (*gs, *arrays, *kept),
        [pl.BlockSpec((3, rows, PIECE), lambda i, half: (0, i, 0))] * count + nine + [pl.BlockSpec(memory_space=pl.ANY)] * len(kept),
        [*nine, pl.BlockSpec((8, 128), lambda i, half: (0, 0))],
        [*[shape(*one.shape, dtype=one.dtype) for one in arrays], shape(8, 128, dtype=F32)],
        grid=(d // rows,),
        half=half,
        aliases={1 + count + 9 + k: k for k in range(len(kept))},
    )


def solution(mesh):
    n = mesh.shape["dp"]
    pair_a = [(i, i + 1 - 2 * (i % 2)) for i in range(n)]
    pair_b = [(i, (i - 1 + 2 * (i % 2)) % n) for i in range(n)]

    def whole_step(x, dy, *arrays):
        weights = arrays[:3]
        layers, _, hidden = weights[0].shape
        pieces = hidden // (2 * PIECE)
        me = lax.axis_index("dp")
        mine = (((me + 1) // 2) % 2).astype(jnp.int32).reshape(1)
        theirs = 1 - mine
        x, dy = x[0], dy[0]
        last = [None]

        def run(f, *args):
            out = f(*args, last[0])
            last[0] = out[-1] if isinstance(out, (tuple, list)) else out
            return out

        def send(array, pairs):
            return lax.ppermute(array, "dp", pairs)

        x_other = send(x, pair_a)
        dy_other = send(dy, pair_a)

        state = {"new": None}
        sums, own_steps, other_steps = [], [], []

        def merge_next():
            layer, piece, part, came = sums.pop(0)
            whole = run(merge, part, came)
            own_steps.append((layer, piece, whole))
            other_steps.append((layer, piece, send(whole, pair_a)))

        def step_next(half, queue, most):
            taken = [queue.pop(0) for _ in range(min(most, len(queue)))]
            layer, start = taken[0][:2]
            state["new"] = run(adamw, half, [one[2] for one in taken], arrays, state["new"], layer, start)[:-1]

        def forward_all(h):
            kept = []
            for layer in range(layers - 1):
                a, at, out = run(forward, h, weights, layer)
                kept.append((h, a, at))
                h = out
            return [*kept, (h, *run(norm, h))]

        def data(side, layer):
            h, a, _ = kept[side][layer]
            return run(data_gradient, h, a, by_h[side][0], weights, layer)

        kept = [forward_all(x), None]
        by_h = [(dy, run(turn, dy)), None]
        next_own = data(0, layers - 1)
        kept[1] = forward_all(x_other)
        by_h[1] = (dy_other, run(turn, dy_other))
        for layer in reversed(range(layers)):
            sides = [(*kept[s][layer][1:], *by_h[s]) for s in range(2)]
            for start in range(0, pieces, GROUP):
                parts = run(weight_gradient, mine, *sides, weights, layer, start, GROUP)
                sums += [(layer, start + k, part, send(part, pair_b)) for k, part in enumerate(parts)]
                if len(sums) > 2:
                    merge_next()
            if layer:
                by_h = [data(0, layer) if layer < layers - 1 else next_own, data(1, layer)]
                merge_next()
                merge_next()
        while sums:
            merge_next()
            for _ in range(2):
                if len(own_steps) >= GROUP:
                    step_next(mine, own_steps, GROUP)
                elif len(other_steps) > GROUP:
                    step_next(theirs, other_steps, GROUP)
        while own_steps:
            step_next(mine, own_steps, GROUP)
        while len(other_steps) > GROUP:
            step_next(theirs, other_steps, GROUP)
        while other_steps:
            step_next(theirs, other_steps, 1)
        return tuple(state["new"])

    return jax.shard_map(
        whole_step,
        mesh=mesh,
        in_specs=(P(("rep", "dp"), None, None),) * 2 + (P(None, None, None),) * 9,
        out_specs=(P("rep", None, None),) * 9,
        check_vma=False,
    )
```

```python
import functools

import jax
import jax.numpy as jnp
from jax import lax
from jax.experimental import pallas as pl
from jax.experimental.pallas import tpu as pltpu
from jax.sharding import PartitionSpec as P


BF16, F32 = jnp.bfloat16, jnp.float32
TOKEN_BLOCK = 512
HIDDEN_BLOCK = 512
PIECE = 256
GROUP = 2
VMEM = 67043328


def nn(a, b):
    return lax.dot_general(a, b, (((1,), (0,)), ((), ())), preferred_element_type=F32)


def nt(a, b):
    return lax.dot_general(a, b, (((1,), (1,)), ((), ())), preferred_element_type=F32)


def scale_of(wide):
    return lax.rsqrt(jnp.mean(wide * wide, -1, keepdims=True) + 1e-6)


def call(kernel, after, ins, in_specs, out_specs, out_shape, *, grid, half=None, with_half=False, scratch=(), aliases=None, cost=0):
    after = [] if after is None else [after]
    scalars = [] if half is None else [half]
    first, last = len(scalars) + len(ins), len(scalars) + len(ins) + len(after)

    def body(*refs):
        kernel(*refs[0 if with_half else len(scalars) : first], *refs[last:])

    return pl.pallas_call(
        body,
        grid_spec=pltpu.PrefetchScalarGridSpec(
            num_scalar_prefetch=len(scalars),
            grid=grid,
            in_specs=[*in_specs, *[pl.BlockSpec(memory_space=pl.ANY)] * len(after)],
            out_specs=out_specs,
            scratch_shapes=scratch,
        ),
        out_shape=out_shape,
        input_output_aliases=aliases or {},
        compiler_params=pltpu.CompilerParams(vmem_limit_bytes=VMEM, dimension_semantics=("arbitrary",)),
        cost_estimate=pl.CostEstimate(flops=1, bytes_accessed=cost, transcendentals=0),
    )(*scalars, *ins, *after)


def shape(*dims, dtype=BF16):
    return jax.ShapeDtypeStruct(dims, dtype)


def weight_specs(layer, d, hidden):
    once = pl.Buffered(1)
    return [
        pl.BlockSpec((None, d, hidden), lambda i: (layer, 0, 0), pipeline_mode=once),
        pl.BlockSpec((None, d, hidden), lambda i: (layer, 0, 0), pipeline_mode=once),
        pl.BlockSpec((None, hidden, d), lambda i: (layer, 0, 0), pipeline_mode=once),
    ]


def normed(h_ref, a_ref, at_ref):
    wide = h_ref[...].astype(F32)
    a = wide * scale_of(wide)
    a_ref[...] = a.astype(BF16)
    at_ref[...] = a.T.astype(BF16)


def forward_kernel(h_ref, wg_ref, wu_ref, wd_ref, a_ref, at_ref, out_ref, *next_refs):
    normed(h_ref, a_ref, at_ref)
    a = a_ref[...]
    hidden = wg_ref.shape[1]
    bf = min(HIDDEN_BLOCK, hidden)
    cols = lambda j: pl.ds(j * bf, bf)
    two = lambda j: (nn(a, wg_ref[:, cols(j)]), nn(a, wu_ref[:, cols(j)]))
    acc, now = None, two(0)
    for j in range(hidden // bf):
        g, u = now
        act = (g * jax.nn.sigmoid(g) * u).astype(BF16)
        if (j + 1) * bf < hidden:
            now = two(j + 1)
        part = nn(act, wd_ref[cols(j), :])
        acc = part if acc is None else acc + part
    out_ref[...] = (h_ref[...].astype(F32) + acc.astype(BF16).astype(F32)).astype(BF16)
    if next_refs:
        normed(out_ref, *next_refs)


def forward(h, weights, layer, also_next, after):
    t, d = h.shape
    tm = min(TOKEN_BLOCK, t)
    row = pl.BlockSpec((tm, d), lambda i: (i, 0))
    col = pl.BlockSpec((d, tm), lambda i: (0, i))
    return call(
        forward_kernel,
        after,
        (h, *weights),
        [row, *weight_specs(layer, d, weights[0].shape[2])],
        [row, col, row] + [row, col] * also_next,
        [shape(t, d), shape(d, t), shape(t, d)] + [shape(t, d), shape(d, t)] * also_next,
        grid=(t // tm,),
    )


def norm(h, after):
    t, d = h.shape
    tm = min(TOKEN_BLOCK, t)
    row = pl.BlockSpec((tm, d), lambda i: (i, 0))
    col = pl.BlockSpec((d, tm), lambda i: (0, i))
    return call(normed, after, (h,), [row], [row, col], [shape(t, d), shape(d, t)], grid=(t // tm,))


def gates(g, u, dact):
    s = jax.nn.sigmoid(g)
    silu = g * s
    act = (silu * u).astype(BF16)
    dact = dact.astype(BF16).astype(F32)
    dg = (dact * u * (s + silu * (1.0 - s))).astype(BF16)
    du = (dact * silu).astype(BF16)
    return act, dg, du


def data_kernel(saved, keep, beside, half_ref, h_ref, a_ref, dy_ref, wg_ref, wu_ref, wd_ref, *refs):
    n_beside = len(beside.ins) if beside else 0
    saved_refs, beside_ins, refs = refs[:saved], refs[saved : saved + n_beside], refs[saved + n_beside :]
    dh_ref, dht_ref, *kept_refs = refs
    if beside:
        kept_refs, beside_outs = kept_refs[:-9], kept_refs[-9:]
        beside.run(beside_ins, beside_outs)
    saved_width = sum(ref.shape[1] for ref in saved_refs[::2])
    a, dy = a_ref[...], dy_ref[...]
    hidden = wg_ref.shape[1]
    bf = min(HIDDEN_BLOCK, hidden)
    blocks = hidden // bf
    if keep:
        kept_refs[0][...] = dy.T

    def cols(j):
        return pl.ds(pl.multiple_of(lax.rem(half_ref[0] * (blocks // 2) + j, blocks) * bf, bf), bf)

    def read(refs, j):
        out, at = [], 0
        for ref in refs:
            if j * bf <= at < (j + 1) * bf:
                out.append(ref[...])
            at += ref.shape[1]
        return jnp.concatenate(out, 1)

    def three(j):
        if j * bf < saved_width:
            return None
        return nn(a, wg_ref[:, cols(j)]), nn(a, wu_ref[:, cols(j)]), nt(dy, wd_ref[cols(j), :])

    acc, now = None, three(0)
    for j in range(blocks):
        if j * bf < saved_width:
            dg, du = read(saved_refs[::2], j), read(saved_refs[1::2], j)
        else:
            act, dg, du = gates(*now)
        if j + 1 < blocks:
            now = three(j + 1)
        if keep and j < blocks // 2:
            for ref, value in zip(kept_refs[1:], (act, dg, du), strict=True):
                ref[:, pl.ds(j * bf, bf)] = value
        part = nt(dg, wg_ref[:, cols(j)]) + nt(du, wu_ref[:, cols(j)])
        acc = part if acc is None else acc + part
    da = acc.astype(BF16).astype(F32)
    wide = h_ref[...].astype(F32)
    scale = scale_of(wide)
    inner = jnp.mean(da * wide, -1, keepdims=True)
    back = (scale * da - wide * (scale * scale * scale * inner)).astype(BF16)
    dh = dy.astype(F32) + back.astype(F32)
    dh_ref[...] = dh.astype(BF16)
    dht_ref[...] = dh.T.astype(BF16)


def data_gradient(half, h, a, dy, weights, layer, saved, keep, jobs, arrays, so_far, after):
    t, d = h.shape
    hidden = weights[0].shape[2]
    tm = min(TOKEN_BLOCK, t)
    row = pl.BlockSpec((tm, d), lambda i, half: (i, 0))
    col = pl.BlockSpec((d, tm), lambda i, half: (0, i))
    once = pl.Buffered(1)
    across = pl.BlockSpec((None, d, hidden), lambda i, half: (layer, 0, 0), pipeline_mode=once)
    down = pl.BlockSpec((None, hidden, d), lambda i, half: (layer, 0, 0), pipeline_mode=once)
    wide = pl.BlockSpec((tm, hidden // 2), lambda i, half: (i, 0))
    ins = [h, a, dy, *weights, *saved]
    specs = [row, row, row, across, across, down] + [pl.BlockSpec((tm, one.shape[1]), lambda i, half: (i, 0)) for one in saved]
    out_specs = [row, col] + [col, wide, wide, wide] * keep
    out_shapes = [shape(t, d), shape(d, t)] + [shape(d, t), *[shape(t, hidden // 2)] * 3] * keep
    aliases = {}
    beside = Beside(jobs, arrays, so_far, t // tm) if jobs else None
    if beside:
        ins += beside.ins
        specs += beside.in_specs
        aliases = {1 + len(ins) - beside.n_kept + k: len(out_specs) + k for k in range(beside.n_kept)}
        out_specs = out_specs + beside.out_specs
        out_shapes = out_shapes + beside.out_shapes
    return call(
        functools.partial(data_kernel, len(saved), keep, beside),
        after,
        ins,
        specs,
        out_specs,
        out_shapes,
        grid=(t // tm,),
        half=half,
        with_half=True,
        aliases=aliases,
    )


def weight_kernel(kinds, count, keep, beside, *refs):
    refs = list(refs)
    take = lambda n: [refs.pop(0) for _ in range(n)]
    sides = [take({"kept": 5, "turned": 4, "plain": 3}[kind]) for kind in kinds]
    wg_ref, wu_ref, wd_ref = take(3)
    beside_ins = take(len(beside.ins)) if beside else None
    outs = take(count)
    beside_outs = take(9) if beside else None
    acc_ref = refs.pop()
    step = pl.program_id(0)

    @pl.when(step == 0)
    def _():
        acc_ref[...] = jnp.zeros_like(acc_ref)

    wg, wu, wd = wg_ref[...], wu_ref[...], wd_ref[...]
    raw = [None if kind == "kept" else (nn(side[0][...], wg), nn(side[0][...], wu), nt(side[2][...], wd)) for kind, side in zip(kinds, sides, strict=True)]
    terms = []
    for kind, side, dots in zip(kinds, sides, raw, strict=True):
        if kind == "kept":
            terms.append([ref[...] for ref in side])
            continue
        act, dg, du = gates(*dots)
        if kind == "turned":
            dyt = side[3][...]
        else:
            dyt = side[2][...].T
            refs.pop(0)[...] = dyt
        if keep:
            refs.pop(0)[...] = dg
            refs.pop(0)[...] = du
        terms.append([side[1][...], dyt, act, dg, du])
    at, dyt = (jnp.concatenate([term[k] for term in terms], 1) for k in range(2))
    act, dg, du = (jnp.concatenate([term[k] for term in terms], 0) for k in range(2, 5))
    acc_ref[0] += nn(at, dg)
    acc_ref[1] += nn(at, du)
    acc_ref[2] += nn(dyt, act)

    if beside:
        beside.run(beside_ins, beside_outs)

    @pl.when(step == pl.num_programs(0) - 1)
    def _():
        for k, out_ref in enumerate(outs):
            out_ref[...] = acc_ref[:, :, k * PIECE : (k + 1) * PIECE].astype(BF16)


def weight_gradient(half, sides, weights, layer, start, count, keep, jobs, arrays, so_far, after):
    d, hidden = weights[0].shape[1:]
    total = hidden // (2 * PIECE)
    t = sides[0][0].size // d
    tm = min(TOKEN_BLOCK if jobs else TOKEN_BLOCK // 2, t)
    row = pl.BlockSpec((tm, d), lambda i, half: (i, 0))
    col = pl.BlockSpec((d, tm), lambda i, half: (0, i))
    width = count * PIECE
    at = lambda half: (half[0] * total + start) // count
    across = pl.BlockSpec((None, d, width), lambda i, half: (layer, 0, at(half)))
    down = pl.BlockSpec((None, width, d), lambda i, half: (layer, at(half), 0))
    block = pl.BlockSpec((tm, width), lambda i, half: (i, start // count))
    first = pl.BlockSpec((tm, width), lambda i, half: (i, 0))
    kinds, specs, more, more_shapes = [], [], [], []
    for side in sides:
        if len(side) == 5:
            kinds.append("kept")
            specs += [col, col, block, block, block]
            continue
        kinds.append("plain" if side[3] is None else "turned")
        specs += [row, col, row] + [col] * (side[3] is not None)
        if side[3] is None:
            more.append(col)
            more_shapes.append(shape(d, t))
        more += [first, first] * keep
        more_shapes += [shape(t, width)] * 2 * keep
    ins = [one for side in sides for one in side if one is not None] + list(weights)
    specs += [across, across, down]
    out_specs, out_shapes, aliases = [pl.BlockSpec((3, d, PIECE), lambda i, half: (0, 0, 0))] * count, [shape(3, d, PIECE)] * count, {}
    beside = Beside(jobs, arrays, so_far, t // tm) if jobs else None
    if beside:
        ins += beside.ins
        specs += beside.in_specs
        aliases = {1 + len(ins) - beside.n_kept + k: count + k for k in range(beside.n_kept)}
        out_specs = out_specs + beside.out_specs
        out_shapes = out_shapes + beside.out_shapes
    return call(
        functools.partial(weight_kernel, kinds, count, keep, beside),
        after,
        ins,
        specs,
        out_specs + more,
        out_shapes + more_shapes,
        grid=(t // tm,),
        half=half,
        aliases=aliases,
        scratch=[pltpu.VMEM((3, d, width), F32)],
    )


def adamw_block(g, w_ref, m_ref, v_ref, new_w_ref, new_m_ref, new_v_ref):
    w = w_ref[...].astype(F32)
    m = 0.9 * m_ref[...] + 0.1 * g
    v = 0.95 * v_ref[...] + 0.05 * g * g
    step = m * lax.rsqrt(v + 1e-8) + 0.1 * w
    new_w_ref[...] = (w - 0.02 * step).astype(BF16)
    new_m_ref[...] = m
    new_v_ref[...] = v


def adamw_kernel(count, *refs):
    gs, ins, token_ref, outs = refs[:count], refs[count : count + 9], refs[-10], refs[-9:]
    token_ref[...] = jnp.zeros_like(token_ref)
    for k in range(3):
        g = jnp.concatenate([g_ref[k].astype(F32) for g_ref in gs], 1)
        adamw_block(g.T if k == 2 else g, *ins[k::3], *outs[k::3])


def adamw(half, gs, arrays, so_far, layer, start, after):
    _, d, _ = gs[0].shape
    count = len(gs)
    total = arrays[0].shape[2] // (2 * PIECE)
    rows = min(256, d)
    width = count * PIECE
    at = lambda half: (half[0] * total + start) // count
    across = pl.BlockSpec((None, rows, width), lambda i, half: (layer, i, at(half)))
    down = pl.BlockSpec((None, width, rows), lambda i, half: (layer, at(half), i))
    nine = [across, across, down] * 3
    kept = [] if so_far is None else list(so_far)
    return call(
        functools.partial(adamw_kernel, count),
        after,
        (*gs, *arrays, *kept),
        [pl.BlockSpec((3, rows, PIECE), lambda i, half: (0, i, 0))] * count + nine + [pl.BlockSpec(memory_space=pl.ANY)] * len(kept),
        [pl.BlockSpec((8, 128), lambda i, half: (0, 0)), *nine],
        [shape(8, 128, dtype=F32), *[shape(*one.shape, dtype=one.dtype) for one in arrays]],
        grid=(d // rows,),
        half=half,
        aliases={1 + count + 9 + k: 1 + k for k in range(len(kept))},
    )


class Beside:
    def __init__(self, jobs, arrays, so_far, steps):
        self.jobs, self.each = jobs, steps // len(jobs)
        self.count = len(jobs[0][1])
        d, hidden = arrays[0].shape[1:]
        total = hidden // (2 * PIECE)
        rows, cols = d // self.each, self.count * PIECE // self.each
        self.split = PIECE // cols
        one = lambda k, i: jnp.clip(i - k * self.each, 0, self.each - 1)

        def pick(i, values):
            out = values[0]
            for k in range(1, len(values)):
                out = jnp.where(i < k * self.each, out, values[k])
            return out

        halves = lambda half: [half[0] if own else 1 - half[0] for own, *_ in jobs]
        layer = lambda i: pick(i, [job[2] for job in jobs])
        group = lambda i, half: pick(i, [(h * total + job[3]) // self.count for h, job in zip(halves(half), jobs, strict=True)])
        across = pl.BlockSpec((None, rows, self.count * PIECE), lambda i, half: (layer(i), i % self.each, group(i, half)))
        down = pl.BlockSpec((None, cols, d), lambda i, half: (layer(i), group(i, half) * self.each + i % self.each, 0))
        nine = [across, across, down] * 3
        kept = [] if so_far is None else list(so_far)
        self.ins, self.in_specs = [], []
        for k, job in enumerate(jobs):
            for g in job[1]:
                self.ins += [g, g]
                self.in_specs.append(pl.BlockSpec((2, rows, PIECE), lambda i, half, k=k: (0, one(k, i), 0)))
                self.in_specs.append(pl.BlockSpec((1, d, cols), lambda i, half, k=k: (2, 0, one(k, i) % self.split)))
        self.ins += [*arrays, *kept]
        self.in_specs += nine + [pl.BlockSpec(memory_space=pl.ANY)] * len(kept)
        self.out_specs = nine
        self.out_shapes = [shape(*a.shape, dtype=a.dtype) for a in arrays]
        self.n_kept = len(kept)

    def run(self, ins, outs):
        step = pl.program_id(0)
        gs = [ins[2 * self.count * k : 2 * self.count * (k + 1)] for k in range(len(self.jobs))]
        nine = ins[2 * self.count * len(self.jobs) :][:9]

        def chosen(of):
            out = of(gs[0])
            for k in range(1, len(gs)):
                out = jnp.where(step < k * self.each, out, of(gs[k]))
            return out

        def third(refs):
            out = refs[1][0].astype(F32)
            for p in range(1, self.count):
                out = jnp.where(lax.rem(step, self.each) // self.split < p, out, refs[2 * p + 1][0].astype(F32))
            return out

        for k in range(2):
            g = chosen(lambda refs, k=k: jnp.concatenate([ref[k].astype(F32) for ref in refs[::2]], 1))
            adamw_block(g, *nine[k::3], *outs[k::3])
        adamw_block(chosen(third).T, *nine[2::3], *outs[2::3])


def adamw_jobs_kernel(beside, *refs):
    ins, token_ref, outs = refs[: len(beside.ins)], refs[-10], refs[-9:]
    token_ref[...] = jnp.zeros_like(token_ref)
    beside.run(ins, outs)


def adamw_jobs(half, jobs, arrays, so_far, after):
    steps = 4 * len(jobs)
    beside = Beside(jobs, arrays, so_far, steps)
    return call(
        functools.partial(adamw_jobs_kernel, beside),
        after,
        beside.ins,
        beside.in_specs,
        [pl.BlockSpec((8, 128), lambda i, half: (0, 0)), *beside.out_specs],
        [shape(8, 128, dtype=F32), *beside.out_shapes],
        grid=(steps,),
        half=half,
        aliases={1 + len(beside.ins) - beside.n_kept + k: 1 + k for k in range(beside.n_kept)},
    )


def solution(mesh):
    n = mesh.shape["dp"]
    pair_a = [(i, i + 1 - 2 * (i % 2)) for i in range(n)]
    pair_b = [(i, (i - 1 + 2 * (i % 2)) % n) for i in range(n)]

    def whole_step(x, dy, *arrays):
        weights = arrays[:3]
        layers, _, hidden = weights[0].shape
        pieces = hidden // (2 * PIECE)
        me = lax.axis_index("dp")
        mine = (((me + 1) // 2) % 2).astype(jnp.int32).reshape(1)
        theirs = 1 - mine
        x, dy = x[0], dy[0]
        last = [None]

        def run(f, *args):
            out = f(*args, last[0])
            last[0] = out[0]
            return out

        def send(array, pairs):
            return lax.ppermute(array, "dp", pairs)

        x_other = send(x, pair_a)
        dy_other = send(dy, pair_a)

        state = {"new": None}
        sums, own_steps, other_steps = [], [], []

        def merge_next():
            layer, piece, part, came = sums.pop(0)
            part, came, _ = lax.optimization_barrier((part, came, last[0]))
            whole = (part.astype(F32) + came.astype(F32)).astype(BF16)
            own_steps.append((layer, piece, whole))
            other_steps.append((layer, piece, send(whole, pair_a)))

        def step_next(half, queue, most):
            taken = [queue.pop(0) for _ in range(min(most, len(queue)))]
            layer, start = taken[0][:2]
            state["new"] = run(adamw, half, [one[2] for one in taken], arrays, state["new"], layer, start)[1:]

        def job(own, queue):
            taken = [queue.pop(0) for _ in range(GROUP)]
            return own, [one[2] for one in taken], *taken[0][:2]

        def forward_all(h):
            kept = []
            for layer in range(layers - 1):
                a, at, out, *following = run(forward, h, weights, layer, layer == layers - 2)
                kept.append((h, a, at))
                h = out
            return [*kept, (h, *(following if layers > 1 else run(norm, h)))]

        def data(side, layer, saved, keep, jobs=()):
            h, a, _ = kept[side][layer]
            out = run(data_gradient, mine, h, a, by_h[side][0], weights, layer, saved, keep, jobs, arrays, state["new"])
            if jobs:
                out, state["new"] = out[: -len(arrays)], out[-len(arrays) :]
            return out

        kept = [forward_all(x), None]
        by_h = [(dy, None), (dy_other, None)]
        next_own, next_own_t, *own_last = data(0, layers - 1, [], True)
        kept[1] = forward_all(x_other)
        for layer in reversed(range(layers)):
            is_last, keep = layer == layers - 1, layer > 0
            saved = [[], []]
            start = 0
            while start < pieces:
                group = 1 if is_last and start < GROUP else GROUP
                sides = [(*kept[s][layer][1:], *by_h[s]) for s in range(2)]
                if is_last:
                    sides[0] = (kept[0][layer][2], *own_last)
                jobs = []
                if not is_last and start == 0 and len(other_steps) >= 2 * GROUP:
                    jobs.append(job(False, other_steps))
                elif not is_last and start == GROUP and len(own_steps) >= GROUP:
                    jobs.append(job(True, own_steps))
                made = run(weight_gradient, mine, sides, weights, layer, start, group, keep, jobs, arrays, state["new"])
                sums += [(layer, start + k, part, send(part, pair_b)) for k, part in enumerate(made[:group])]
                if jobs:
                    state["new"] = made[group : group + len(arrays)]
                made = list(made[group + (len(arrays) if jobs else 0) :])
                for s in range(2):
                    if len(sides[s]) == 4:
                        if sides[s][3] is None:
                            by_h[s] = (by_h[s][0], made.pop(0))
                        if keep:
                            saved[s] += [made.pop(0), made.pop(0)]
                while len(sums) > (3 if is_last or start else 2):
                    merge_next()
                if not is_last and start == GROUP:
                    if len(own_steps) >= GROUP:
                        state["new"] = run(adamw_jobs, mine, [job(True, own_steps)], arrays, state["new"])[1:]
                    merge_next()
                start += group
            if layer:
                own = (next_own, next_own_t) if is_last else data(0, layer, saved[0], False)
                jobs = [job(True, own_steps)] if len(own_steps) >= GROUP else []
                by_h = [own, data(1, layer, saved[1], False, jobs)]
                while len(sums) > 1:
                    merge_next()

        def steps_now():
            jobs = [job(True, own_steps)] if len(own_steps) >= GROUP else []
            if len(other_steps) >= 2 * GROUP:
                jobs.append(job(False, other_steps))
            if jobs:
                state["new"] = run(adamw_jobs, mine, jobs, arrays, state["new"])[1:]
            return jobs

        steps_now()
        while sums:
            merge_next()
            steps_now()
        while steps_now():
            pass
        while other_steps:
            step_next(theirs, other_steps, 1)
        return tuple(state["new"])

    return jax.shard_map(
        whole_step,
        mesh=mesh,
        in_specs=(P(("rep", "dp"), None, None),) * 2 + (P(None, None, None),) * 9,
        out_specs=(P("rep", None, None),) * 9,
        check_vma=False,
    )
```

```python
import functools

import jax
import jax.numpy as jnp
from jax import lax
from jax.experimental import pallas as pl
from jax.experimental.pallas import tpu as pltpu
from jax.sharding import PartitionSpec as P


BF16, F32 = jnp.bfloat16, jnp.float32
TOKEN_BLOCK = 512
HIDDEN_BLOCK = 512
PIECE = 256
GROUP = 2
VMEM = 67043328


def nn(a, b):
    return lax.dot_general(a, b, (((1,), (0,)), ((), ())), preferred_element_type=F32)


def nt(a, b):
    return lax.dot_general(a, b, (((1,), (1,)), ((), ())), preferred_element_type=F32)


def scale_of(wide):
    return lax.rsqrt(jnp.mean(wide * wide, -1, keepdims=True) + 1e-6)


def call(kernel, after, ins, in_specs, out_specs, out_shape, *, grid, half=None, with_half=False, scratch=(), aliases=None, cost=0):
    after = [] if after is None else [after]
    scalars = [] if half is None else [half]
    first, last = len(scalars) + len(ins), len(scalars) + len(ins) + len(after)

    def body(*refs):
        kernel(*refs[0 if with_half else len(scalars) : first], *refs[last:])

    return pl.pallas_call(
        body,
        grid_spec=pltpu.PrefetchScalarGridSpec(
            num_scalar_prefetch=len(scalars),
            grid=grid,
            in_specs=[*in_specs, *[pl.BlockSpec(memory_space=pl.ANY)] * len(after)],
            out_specs=out_specs,
            scratch_shapes=scratch,
        ),
        out_shape=out_shape,
        input_output_aliases=aliases or {},
        compiler_params=pltpu.CompilerParams(vmem_limit_bytes=VMEM, dimension_semantics=("arbitrary",)),
        cost_estimate=pl.CostEstimate(flops=1, bytes_accessed=cost, transcendentals=0),
    )(*scalars, *ins, *after)


def shape(*dims, dtype=BF16):
    return jax.ShapeDtypeStruct(dims, dtype)


def weight_specs(layer, d, hidden):
    once = pl.Buffered(1)
    return [
        pl.BlockSpec((None, d, hidden), lambda i: (layer, 0, 0), pipeline_mode=once),
        pl.BlockSpec((None, d, hidden), lambda i: (layer, 0, 0), pipeline_mode=once),
        pl.BlockSpec((None, hidden, d), lambda i: (layer, 0, 0), pipeline_mode=once),
    ]


def normed(h_ref, a_ref, at_ref):
    wide = h_ref[...].astype(F32)
    a = wide * scale_of(wide)
    a_ref[...] = a.astype(BF16)
    at_ref[...] = a.T.astype(BF16)


def forward_kernel(h_ref, wg_ref, wu_ref, wd_ref, a_ref, at_ref, out_ref, *next_refs):
    normed(h_ref, a_ref, at_ref)
    a = a_ref[...]
    hidden = wg_ref.shape[1]
    bf = min(HIDDEN_BLOCK, hidden)
    cols = lambda j: pl.ds(j * bf, bf)
    two = lambda j: (nn(a, wg_ref[:, cols(j)]), nn(a, wu_ref[:, cols(j)]))
    acc, now = None, two(0)
    for j in range(hidden // bf):
        g, u = now
        act = (g * jax.nn.sigmoid(g) * u).astype(BF16)
        if (j + 1) * bf < hidden:
            now = two(j + 1)
        part = nn(act, wd_ref[cols(j), :])
        acc = part if acc is None else acc + part
    out_ref[...] = (h_ref[...].astype(F32) + acc.astype(BF16).astype(F32)).astype(BF16)
    if next_refs:
        normed(out_ref, *next_refs)


def forward(h, weights, layer, also_next, after):
    t, d = h.shape
    tm = min(TOKEN_BLOCK, t)
    row = pl.BlockSpec((tm, d), lambda i: (i, 0))
    col = pl.BlockSpec((d, tm), lambda i: (0, i))
    return call(
        forward_kernel,
        after,
        (h, *weights),
        [row, *weight_specs(layer, d, weights[0].shape[2])],
        [row, col, row] + [row, col] * also_next,
        [shape(t, d), shape(d, t), shape(t, d)] + [shape(t, d), shape(d, t)] * also_next,
        grid=(t // tm,),
    )


def norm(h, after):
    t, d = h.shape
    tm = min(TOKEN_BLOCK, t)
    row = pl.BlockSpec((tm, d), lambda i: (i, 0))
    col = pl.BlockSpec((d, tm), lambda i: (0, i))
    return call(normed, after, (h,), [row], [row, col], [shape(t, d), shape(d, t)], grid=(t // tm,))


def gates(g, u, dact):
    s = jax.nn.sigmoid(g)
    silu = g * s
    act = (silu * u).astype(BF16)
    dact = dact.astype(BF16).astype(F32)
    dg = (dact * u * (s + silu * (1.0 - s))).astype(BF16)
    du = (dact * silu).astype(BF16)
    return act, dg, du


def data_kernel(saved, keep, beside, half_ref, h_ref, a_ref, dy_ref, wg_ref, wu_ref, wd_ref, *refs):
    n_beside = len(beside.ins) if beside else 0
    saved_refs, beside_ins, refs = refs[:saved], refs[saved : saved + n_beside], refs[saved + n_beside :]
    dh_ref, dht_ref, *kept_refs = refs
    if beside:
        kept_refs, beside_outs = kept_refs[:-9], kept_refs[-9:]
        beside.run(beside_ins, beside_outs)
    saved_width = sum(ref.shape[1] for ref in saved_refs[::2])
    a, dy = a_ref[...], dy_ref[...]
    hidden = wg_ref.shape[1]
    bf = min(HIDDEN_BLOCK, hidden)
    blocks = hidden // bf
    if keep:
        kept_refs[0][...] = dy.T

    def cols(j):
        return pl.ds(pl.multiple_of(lax.rem(half_ref[0] * (blocks // 2) + j, blocks) * bf, bf), bf)

    def read(refs, j):
        out, at = [], 0
        for ref in refs:
            if j * bf <= at < (j + 1) * bf:
                out.append(ref[...])
            at += ref.shape[1]
        return jnp.concatenate(out, 1)

    def three(j):
        if j * bf < saved_width:
            return None
        return nn(a, wg_ref[:, cols(j)]), nn(a, wu_ref[:, cols(j)]), nt(dy, wd_ref[cols(j), :])

    acc, now = None, three(0)
    for j in range(blocks):
        if j * bf < saved_width:
            dg, du = read(saved_refs[::2], j), read(saved_refs[1::2], j)
        else:
            act, dg, du = gates(*now)
        if j + 1 < blocks:
            now = three(j + 1)
        if keep and j < blocks // 2:
            for ref, value in zip(kept_refs[1:], (act, dg, du), strict=True):
                ref[:, pl.ds(j * bf, bf)] = value
        part = nt(dg, wg_ref[:, cols(j)]) + nt(du, wu_ref[:, cols(j)])
        acc = part if acc is None else acc + part
    da = acc.astype(BF16).astype(F32)
    wide = h_ref[...].astype(F32)
    scale = scale_of(wide)
    inner = jnp.mean(da * wide, -1, keepdims=True)
    back = (scale * da - wide * (scale * scale * scale * inner)).astype(BF16)
    dh = dy.astype(F32) + back.astype(F32)
    dh_ref[...] = dh.astype(BF16)
    dht_ref[...] = dh.T.astype(BF16)


def data_gradient(half, h, a, dy, weights, layer, saved, keep, jobs, arrays, so_far, after):
    t, d = h.shape
    hidden = weights[0].shape[2]
    tm = min(TOKEN_BLOCK, t)
    row = pl.BlockSpec((tm, d), lambda i, half: (i, 0))
    col = pl.BlockSpec((d, tm), lambda i, half: (0, i))
    once = pl.Buffered(1)
    across = pl.BlockSpec((None, d, hidden), lambda i, half: (layer, 0, 0), pipeline_mode=once)
    down = pl.BlockSpec((None, hidden, d), lambda i, half: (layer, 0, 0), pipeline_mode=once)
    wide = pl.BlockSpec((tm, hidden // 2), lambda i, half: (i, 0))
    ins = [h, a, dy, *weights, *saved]
    specs = [row, row, row, across, across, down] + [pl.BlockSpec((tm, one.shape[1]), lambda i, half: (i, 0)) for one in saved]
    out_specs = [row, col] + [col, wide, wide, wide] * keep
    out_shapes = [shape(t, d), shape(d, t)] + [shape(d, t), *[shape(t, hidden // 2)] * 3] * keep
    aliases = {}
    beside = Beside(jobs, arrays, so_far, t // tm) if jobs else None
    if beside:
        ins += beside.ins
        specs += beside.in_specs
        aliases = {1 + len(ins) - beside.n_kept + k: len(out_specs) + k for k in range(beside.n_kept)}
        out_specs = out_specs + beside.out_specs
        out_shapes = out_shapes + beside.out_shapes
    return call(
        functools.partial(data_kernel, len(saved), keep, beside),
        after,
        ins,
        specs,
        out_specs,
        out_shapes,
        grid=(t // tm,),
        half=half,
        with_half=True,
        aliases=aliases,
    )


def weight_kernel(kinds, count, keep, beside, *refs):
    refs = list(refs)
    take = lambda n: [refs.pop(0) for _ in range(n)]
    sides = [take({"kept": 5, "turned": 4, "plain": 3}[kind]) for kind in kinds]
    wg_ref, wu_ref, wd_ref = take(3)
    beside_ins = take(len(beside.ins)) if beside else None
    outs = take(count)
    beside_outs = take(9) if beside else None
    acc_ref = refs.pop()
    step = pl.program_id(0)

    @pl.when(step == 0)
    def _():
        acc_ref[...] = jnp.zeros_like(acc_ref)

    wg, wu, wd = wg_ref[...], wu_ref[...], wd_ref[...]
    raw = [None if kind == "kept" else (nn(side[0][...], wg), nn(side[0][...], wu), nt(side[2][...], wd)) for kind, side in zip(kinds, sides, strict=True)]
    terms = []
    for kind, side, dots in zip(kinds, sides, raw, strict=True):
        if kind == "kept":
            terms.append([ref[...] for ref in side])
            continue
        act, dg, du = gates(*dots)
        if kind == "turned":
            dyt = side[3][...]
        else:
            dyt = side[2][...].T
            refs.pop(0)[...] = dyt
        if keep:
            refs.pop(0)[...] = dg
            refs.pop(0)[...] = du
        terms.append([side[1][...], dyt, act, dg, du])
    at, dyt = (jnp.concatenate([term[k] for term in terms], 1) for k in range(2))
    act, dg, du = (jnp.concatenate([term[k] for term in terms], 0) for k in range(2, 5))
    acc_ref[0] += nn(at, dg)
    acc_ref[1] += nn(at, du)
    acc_ref[2] += nn(dyt, act)

    if beside:
        beside.run(beside_ins, beside_outs)

    @pl.when(step == pl.num_programs(0) - 1)
    def _():
        for k, out_ref in enumerate(outs):
            out_ref[...] = acc_ref[:, :, k * PIECE : (k + 1) * PIECE].astype(BF16)


def weight_gradient(half, sides, weights, layer, start, count, keep, jobs, arrays, so_far, after):
    d, hidden = weights[0].shape[1:]
    total = hidden // (2 * PIECE)
    t = sides[0][0].size // d
    tm = min(TOKEN_BLOCK if jobs else TOKEN_BLOCK // 2, t)
    row = pl.BlockSpec((tm, d), lambda i, half: (i, 0))
    col = pl.BlockSpec((d, tm), lambda i, half: (0, i))
    width = count * PIECE
    at = lambda half: (half[0] * total + start) // count
    across = pl.BlockSpec((None, d, width), lambda i, half: (layer, 0, at(half)))
    down = pl.BlockSpec((None, width, d), lambda i, half: (layer, at(half), 0))
    block = pl.BlockSpec((tm, width), lambda i, half: (i, start // count))
    first = pl.BlockSpec((tm, width), lambda i, half: (i, 0))
    kinds, specs, more, more_shapes = [], [], [], []
    for side in sides:
        if len(side) == 5:
            kinds.append("kept")
            specs += [col, col, block, block, block]
            continue
        kinds.append("plain" if side[3] is None else "turned")
        specs += [row, col, row] + [col] * (side[3] is not None)
        if side[3] is None:
            more.append(col)
            more_shapes.append(shape(d, t))
        more += [first, first] * keep
        more_shapes += [shape(t, width)] * 2 * keep
    ins = [one for side in sides for one in side if one is not None] + list(weights)
    specs += [across, across, down]
    out_specs, out_shapes, aliases = [pl.BlockSpec((3, d, PIECE), lambda i, half: (0, 0, 0))] * count, [shape(3, d, PIECE)] * count, {}
    beside = Beside(jobs, arrays, so_far, t // tm) if jobs else None
    if beside:
        ins += beside.ins
        specs += beside.in_specs
        aliases = {1 + len(ins) - beside.n_kept + k: count + k for k in range(beside.n_kept)}
        out_specs = out_specs + beside.out_specs
        out_shapes = out_shapes + beside.out_shapes
    return call(
        functools.partial(weight_kernel, kinds, count, keep, beside),
        after,
        ins,
        specs,
        out_specs + more,
        out_shapes + more_shapes,
        grid=(t // tm,),
        half=half,
        aliases=aliases,
        scratch=[pltpu.VMEM((3, d, width), F32)],
    )


def adamw_block(g, w_ref, m_ref, v_ref, new_w_ref, new_m_ref, new_v_ref):
    w = w_ref[...].astype(F32)
    m = 0.9 * m_ref[...] + 0.1 * g
    v = 0.95 * v_ref[...] + 0.05 * g * g
    step = m * lax.rsqrt(v + 1e-8) + 0.1 * w
    new_w_ref[...] = (w - 0.02 * step).astype(BF16)
    new_m_ref[...] = m
    new_v_ref[...] = v


def adamw_kernel(count, *refs):
    gs, ins, token_ref, outs = refs[:count], refs[count : count + 9], refs[-10], refs[-9:]
    token_ref[...] = jnp.zeros_like(token_ref)
    for k in range(3):
        g = jnp.concatenate([g_ref[k].astype(F32) for g_ref in gs], 1)
        adamw_block(g.T if k == 2 else g, *ins[k::3], *outs[k::3])


def adamw(half, gs, arrays, so_far, layer, start, after):
    _, d, _ = gs[0].shape
    count = len(gs)
    total = arrays[0].shape[2] // (2 * PIECE)
    rows = min(256, d)
    width = count * PIECE
    at = lambda half: (half[0] * total + start) // count
    across = pl.BlockSpec((None, rows, width), lambda i, half: (layer, i, at(half)))
    down = pl.BlockSpec((None, width, rows), lambda i, half: (layer, at(half), i))
    nine = [across, across, down] * 3
    kept = [] if so_far is None else list(so_far)
    return call(
        functools.partial(adamw_kernel, count),
        after,
        (*gs, *arrays, *kept),
        [pl.BlockSpec((3, rows, PIECE), lambda i, half: (0, i, 0))] * count + nine + [pl.BlockSpec(memory_space=pl.ANY)] * len(kept),
        [pl.BlockSpec((8, 128), lambda i, half: (0, 0)), *nine],
        [shape(8, 128, dtype=F32), *[shape(*one.shape, dtype=one.dtype) for one in arrays]],
        grid=(d // rows,),
        half=half,
        aliases={1 + count + 9 + k: 1 + k for k in range(len(kept))},
    )


class Beside:
    def __init__(self, jobs, arrays, so_far, steps):
        self.jobs, self.each = jobs, steps // len(jobs)
        self.count = len(jobs[0][1])
        d, hidden = arrays[0].shape[1:]
        total = hidden // (2 * PIECE)
        rows, cols = d // self.each, self.count * PIECE // self.each
        self.split = PIECE // cols
        one = lambda k, i: jnp.clip(i - k * self.each, 0, self.each - 1)

        def pick(i, values):
            out = values[0]
            for k in range(1, len(values)):
                out = jnp.where(i < k * self.each, out, values[k])
            return out

        halves = lambda half: [half[0] if own else 1 - half[0] for own, *_ in jobs]
        layer = lambda i: pick(i, [job[2] for job in jobs])
        group = lambda i, half: pick(i, [(h * total + job[3]) // self.count for h, job in zip(halves(half), jobs, strict=True)])
        across = pl.BlockSpec((None, rows, self.count * PIECE), lambda i, half: (layer(i), i % self.each, group(i, half)))
        down = pl.BlockSpec((None, cols, d), lambda i, half: (layer(i), group(i, half) * self.each + i % self.each, 0))
        nine = [across, across, down] * 3
        kept = [] if so_far is None else list(so_far)
        self.ins, self.in_specs = [], []
        for k, job in enumerate(jobs):
            for g in job[1]:
                self.ins += [g, g]
                self.in_specs.append(pl.BlockSpec((2, rows, PIECE), lambda i, half, k=k: (0, one(k, i), 0)))
                self.in_specs.append(pl.BlockSpec((1, d, cols), lambda i, half, k=k: (2, 0, one(k, i) % self.split)))
        self.ins += [*arrays, *kept]
        self.in_specs += nine + [pl.BlockSpec(memory_space=pl.ANY)] * len(kept)
        self.out_specs = nine
        self.out_shapes = [shape(*a.shape, dtype=a.dtype) for a in arrays]
        self.n_kept = len(kept)

    def run(self, ins, outs):
        step = pl.program_id(0)
        gs = [ins[2 * self.count * k : 2 * self.count * (k + 1)] for k in range(len(self.jobs))]
        nine = ins[2 * self.count * len(self.jobs) :][:9]

        def chosen(of):
            out = of(gs[0])
            for k in range(1, len(gs)):
                out = jnp.where(step < k * self.each, out, of(gs[k]))
            return out

        def third(refs):
            out = refs[1][0].astype(F32)
            for p in range(1, self.count):
                out = jnp.where(lax.rem(step, self.each) // self.split < p, out, refs[2 * p + 1][0].astype(F32))
            return out

        for k in range(2):
            g = chosen(lambda refs, k=k: jnp.concatenate([ref[k].astype(F32) for ref in refs[::2]], 1))
            adamw_block(g, *nine[k::3], *outs[k::3])
        adamw_block(chosen(third).T, *nine[2::3], *outs[2::3])


def adamw_jobs_kernel(beside, *refs):
    ins, token_ref, outs = refs[: len(beside.ins)], refs[-10], refs[-9:]
    token_ref[...] = jnp.zeros_like(token_ref)
    beside.run(ins, outs)


def adamw_jobs(half, jobs, arrays, so_far, after):
    steps = 2 * len(jobs)
    beside = Beside(jobs, arrays, so_far, steps)
    return call(
        functools.partial(adamw_jobs_kernel, beside),
        after,
        beside.ins,
        beside.in_specs,
        [pl.BlockSpec((8, 128), lambda i, half: (0, 0)), *beside.out_specs],
        [shape(8, 128, dtype=F32), *beside.out_shapes],
        grid=(steps,),
        half=half,
        aliases={1 + len(beside.ins) - beside.n_kept + k: 1 + k for k in range(beside.n_kept)},
    )


def solution(mesh):
    n = mesh.shape["dp"]
    pair_a = [(i, i + 1 - 2 * (i % 2)) for i in range(n)]
    pair_b = [(i, (i - 1 + 2 * (i % 2)) % n) for i in range(n)]

    def whole_step(x, dy, *arrays):
        weights = arrays[:3]
        layers, _, hidden = weights[0].shape
        pieces = hidden // (2 * PIECE)
        me = lax.axis_index("dp")
        mine = (((me + 1) // 2) % 2).astype(jnp.int32).reshape(1)
        theirs = 1 - mine
        x, dy = x[0], dy[0]
        last = [None]

        def run(f, *args):
            out = f(*args, last[0])
            last[0] = out[0]
            return out

        def send(array, pairs):
            return lax.ppermute(array, "dp", pairs)

        x_other = send(x, pair_a)
        dy_other = send(dy, pair_a)

        state = {"new": None}
        sums, own_steps, other_steps = [], [], []

        def merge_next():
            layer, piece, part, came = sums.pop(0)
            part, came, _ = lax.optimization_barrier((part, came, last[0]))
            whole = (part.astype(F32) + came.astype(F32)).astype(BF16)
            own_steps.append((layer, piece, whole))
            other_steps.append((layer, piece, send(whole, pair_a)))

        def step_next(half, queue, most):
            taken = [queue.pop(0) for _ in range(min(most, len(queue)))]
            layer, start = taken[0][:2]
            state["new"] = run(adamw, half, [one[2] for one in taken], arrays, state["new"], layer, start)[1:]

        def job(own, queue):
            taken = [queue.pop(0) for _ in range(GROUP)]
            return own, [one[2] for one in taken], *taken[0][:2]

        def forward_all(h):
            kept = []
            for layer in range(layers - 1):
                a, at, out, *following = run(forward, h, weights, layer, layer == layers - 2)
                kept.append((h, a, at))
                h = out
            return [*kept, (h, *(following if layers > 1 else run(norm, h)))]

        def data(side, layer, saved, keep, jobs=()):
            h, a, _ = kept[side][layer]
            out = run(data_gradient, mine, h, a, by_h[side][0], weights, layer, saved, keep, jobs, arrays, state["new"])
            if jobs:
                out, state["new"] = out[: -len(arrays)], out[-len(arrays) :]
            return out

        kept = [forward_all(x), None]
        by_h = [(dy, None), (dy_other, None)]
        next_own, next_own_t, *own_last = data(0, layers - 1, [], True)
        kept[1] = forward_all(x_other)
        for layer in reversed(range(layers)):
            is_last, keep = layer == layers - 1, layer > 0
            saved = [[], []]
            start = 0
            while start < pieces:
                group = GROUP
                sides = [(*kept[s][layer][1:], *by_h[s]) for s in range(2)]
                if is_last:
                    sides[0] = (kept[0][layer][2], *own_last)
                jobs = []
                if not is_last and start == 0 and len(other_steps) >= 2 * GROUP:
                    jobs.append(job(False, other_steps))
                made = run(weight_gradient, mine, sides, weights, layer, start, group, keep, jobs, arrays, state["new"])
                sums += [(layer, start + k, part, send(part, pair_b)) for k, part in enumerate(made[:group])]
                if jobs:
                    state["new"] = made[group : group + len(arrays)]
                made = list(made[group + (len(arrays) if jobs else 0) :])
                for s in range(2):
                    if len(sides[s]) == 4:
                        if sides[s][3] is None:
                            by_h[s] = (by_h[s][0], made.pop(0))
                        if keep:
                            saved[s] += [made.pop(0), made.pop(0)]
                left = 2 if not is_last and start == 0 else 3
                if is_last and start + group >= pieces:
                    while len(sums) > left + 1:
                        merge_next()
                    if len(own_steps) >= GROUP:
                        state["new"] = run(adamw_jobs, mine, [job(True, own_steps)], arrays, state["new"])[1:]
                while len(sums) > left:
                    merge_next()
                if not is_last and start == GROUP:
                    if len(own_steps) >= GROUP:
                        state["new"] = run(adamw_jobs, mine, [job(True, own_steps)], arrays, state["new"])[1:]
                    merge_next()
                start += group
            if layer:
                own = (next_own, next_own_t) if is_last else data(0, layer, saved[0], False)
                jobs = [job(True, own_steps)] if len(own_steps) >= GROUP else []
                by_h = [own, data(1, layer, saved[1], False, jobs)]
                while len(sums) > 1:
                    merge_next()

        def steps_now():
            jobs = [job(True, own_steps)] if len(own_steps) >= GROUP else []
            if len(other_steps) >= 2 * GROUP:
                jobs.append(job(False, other_steps))
            if jobs:
                state["new"] = run(adamw_jobs, mine, jobs, arrays, state["new"])[1:]
            return jobs

        steps_now()
        while sums:
            merge_next()
            steps_now()
        while steps_now():
            pass
        while other_steps:
            step_next(theirs, other_steps, 1)
        return tuple(state["new"])

    return jax.shard_map(
        whole_step,
        mesh=mesh,
        in_specs=(P(("rep", "dp"), None, None),) * 2 + (P(None, None, None),) * 9,
        out_specs=(P("rep", None, None),) * 9,
        check_vma=False,
    )
```
